512 devices in a mesh: clip: 2 (over y), outer: 32 (over z), inner: 4 (over x), head: 2 (over core).
Axes of the slice: x: 4, y: 2, z: 32, core: 2. Of those that a mesh axis runs over, the one named last changes fastest.
The devices are a block of a 4x8x32 slice.
Arguments:
- tokens: bfloat16 [2, 4096, 3072], P('clip', ('outer', 'inner', 'head')), parts along dimension 0, may hold values from -6 to 6
- shift_mod: float32 [2, 3072], P('clip'), parts along dimension 0, may hold values from -3 to 3
- scale_mod: float32 [2, 3072], P('clip'), parts along dimension 0, may hold values from -1.5 to 1.5
- gate_mod: float32 [2, 3072], P('clip'), parts along dimension 0, may hold values from 0.5 to 2
- query_weight: bfloat16 [3072, 3072], P('outer', ('inner', 'head')), may hold values from -0.109375 to 0.109375
- key_weight: bfloat16 [3072, 3072], P('outer', ('inner', 'head')), may hold values from -0.109375 to 0.109375
- value_weight: bfloat16 [3072, 3072], P('outer', ('inner', 'head')), may hold values from -0.109375 to 0.109375
- out_weight: bfloat16 [3072, 3072], P(('inner', 'head'), 'outer'), may hold values from -0.109375 to 0.109375
- query_gain: float32 [128], replicated, may hold values from 1 to 18, as said below
- key_gain: float32 [128], replicated, may hold values from 1 to 18, as said below
Outputs:
- attended: bfloat16 [2, 4096, 3072], P('clip', ('outer', 'inner', 'head')), parts along dimension 0
The draws below stay inside these ranges and needn't reach their ends.
There are 2 independent parts, one for each index of `clip`. The reference program is written for one: setup_inputs(seed, part) draws one part's arguments, and reference() takes and returns one part's arrays. A program takes and returns all parts, laid end to end along the dimension named above; an argument that names none is the same for every part. Nothing has to cross between parts.
Inputs may be any that keep to these rules, and one draw needn't show every extreme that they name: `query_gain`: 128 positive scales. `key_gain`: 128 positive scales.
All inputs are finite; a program needn't handle non-finite values.
Results may differ from the reference program's by a relative error of at most 0.015.
The reference program's roundings to bfloat16 on the way (of `modulated`, `value_heads`, `mixed` and `group_term`) count: a program that leaves them out, or rounds other values in their place, can miss the bound.
Values may be sent and summed in bfloat16 or wider, within the bound.
No kernel may reach another device: no remote copies, remote signals or barrier semaphores. Data moves between devices by JAX's collectives and lax.ppermute only.
A program may use at most 64 MiB of HBM per device.

```python
import math
import jax
import jax.numpy as jnp
from jax import lax

D = 3072
HEADS = 24
HD = 128
S = 4096
CLIPS = 1
N_INNER = 4
N_HEAD = 2


def base_gain(key):
    lower_log = jnp.log(jnp.float32(1.0))
    upper_log = jnp.log(jnp.float32(2.0))
    return jnp.exp(jax.random.uniform(key, (HD,), jnp.float32, lower_log, upper_log))


def draw_query_gain(key, part):
    gain_values = base_gain(jax.random.fold_in(key, 1))
    return gain_values


def draw_key_gain(key, part):
    gain_values = base_gain(jax.random.fold_in(key, 2))
    return gain_values


def levels(stream_key, dims, cuts, least, high):
    factor_of = 1.0
    for position, shards_of in cuts:
        steps = jax.random.uniform(jax.random.fold_in(jax.random.fold_in(stream_key, 6), position), (shards_of,), jnp.float32, least / len(cuts), high / len(cuts))
        factor_of = factor_of * jnp.repeat(jnp.exp(steps), dims[position] // shards_of).reshape((-1,) + (1,) * (len(dims) - 1 - position))
    return factor_of


def noise(rng, dims, scale, limit, shards=(), held_as=jnp.bfloat16):
    entries = jax.random.normal(rng, dims, jnp.float32) * scale
    if len(shards) > 0:
        entries = levels(rng, dims, shards, -0.22, 0.18) * entries
    return jnp.clip(entries, min=-limit, max=limit).astype(held_as)


def setup_inputs(seed: int = 0, part: int = 0) -> dict:
    keys = jax.random.split(jax.random.key(seed), 11)
    own_keys = jax.random.split(jax.random.fold_in(keys[10], part), 11)
    return {
        "tokens": noise(own_keys[0], (CLIPS, S, D), 1.0, 6.0, ((1, 256),)),
        "shift_mod": noise(own_keys[1], (CLIPS, D), 0.5, 3.0, (), jnp.float32),
        "scale_mod": noise(own_keys[2], (CLIPS, D), 0.3, 1.5, (), jnp.float32),
        "gate_mod": jnp.clip(jax.random.uniform(own_keys[3], (CLIPS, D), jnp.float32, 0.5, 2.0), 0.5, 2.0),
        "query_weight": noise(keys[4], (D, HEADS * HD), D ** -0.5, 0.109375, ((0, 32), (1, 8))),
        "key_weight": noise(keys[5], (D, HEADS * HD), D ** -0.5, 0.109375, ((0, 32), (1, 8))),
        "value_weight": noise(keys[6], (D, HEADS * HD), D ** -0.5, 0.109375, ((0, 32), (1, 8))),
        "out_weight": noise(keys[7], (HEADS * HD, D), (HEADS * HD) ** -0.5, 0.109375, ((0, 8), (1, 32))),
        "query_gain": draw_query_gain(jax.random.fold_in(keys[10], 71), part),
        "key_gain": draw_key_gain(jax.random.fold_in(keys[10], 71), part),
    }


EPSILON = 1e-06

def modulate(tokens, shift_mod, scale_mod):
    values = tokens.astype(jnp.float32)
    center = lax.optimization_barrier(jnp.mean(values, axis=-1, keepdims=True))
    spread = lax.optimization_barrier(jnp.mean(jnp.square(values - center), axis=-1, keepdims=True))
    normed = (values - center) / jnp.sqrt(spread + EPSILON)
    return (normed * (1.0 + scale_mod[:, None, :]) + shift_mod[:, None, :]).astype(jnp.bfloat16)

def head_norm(projected, gain_vec, head_dim):
    shaped = projected.reshape(projected.shape[:-1] + (projected.shape[-1] // head_dim, head_dim))
    mean_square = lax.optimization_barrier(jnp.mean(jnp.square(shaped), axis=-1, keepdims=True))
    return (shaped / jnp.sqrt(mean_square + EPSILON) * gain_vec).astype(jnp.bfloat16)

def one_head(operands):
    query_one, key_one, value_one = operands
    scores = jnp.einsum('cqd,ckd->cqk', query_one.astype(jnp.float32), key_one.astype(jnp.float32), precision=lax.Precision.HIGHEST) / math.sqrt(HD)
    row_max = lax.optimization_barrier(jnp.max(scores, axis=-1, keepdims=True))
    weights = jnp.exp(scores - row_max)
    row_total = lax.optimization_barrier(jnp.sum(weights, axis=-1, keepdims=True))
    rounded = lax.optimization_barrier(weights.astype(jnp.bfloat16))
    mixed_values = jnp.einsum('cqk,ckd->cqd', rounded.astype(jnp.float32), value_one.astype(jnp.float32), precision=lax.Precision.HIGHEST)
    return mixed_values / row_total

def reference(tokens, shift_mod, scale_mod, gate_mod, query_weight, key_weight, value_weight, out_weight, query_gain, key_gain):
    clip_count = tokens.shape[0]
    all_cols = HEADS * HD
    modulated = modulate(tokens, shift_mod, scale_mod).reshape(clip_count * S, D)
    query_proj = jnp.dot(modulated, query_weight, preferred_element_type=jnp.float32)
    key_proj = jnp.dot(modulated, key_weight, preferred_element_type=jnp.float32)
    value_proj = jnp.dot(modulated, value_weight, preferred_element_type=jnp.float32)
    query_heads = lax.optimization_barrier(head_norm(query_proj.reshape(clip_count, S, all_cols), query_gain, HD))
    key_heads = lax.optimization_barrier(head_norm(key_proj.reshape(clip_count, S, all_cols), key_gain, HD))
    value_heads = lax.optimization_barrier(value_proj.astype(jnp.bfloat16).reshape(clip_count, S, HEADS, HD))
    stacked = (jnp.transpose(query_heads, (2, 0, 1, 3)), jnp.transpose(key_heads, (2, 0, 1, 3)), jnp.transpose(value_heads, (2, 0, 1, 3)))
    head_out = lax.map(one_head, stacked)
    mixed = jnp.transpose(head_out, (1, 2, 0, 3)).reshape(clip_count * S, all_cols).astype(jnp.bfloat16)
    groups = N_INNER * N_HEAD
    group_width = all_cols // groups
    summed = jnp.zeros((clip_count * S, D), jnp.float32)
    for group_index in range(groups):
        lower = group_index * group_width
        group_term = jnp.dot(mixed[:, lower:lower + group_width], out_weight[lower:lower + group_width, :], preferred_element_type=jnp.float32).astype(jnp.bfloat16)
        group_term = lax.optimization_barrier(group_term)
        summed = summed + group_term.astype(jnp.float32)
    return (summed.reshape(clip_count, S, D) * gate_mod[:, None, :]).astype(jnp.bfloat16)
```

```python
import math

import jax
import jax.numpy as jnp
from jax import lax
from jax.experimental import pallas as pl
from jax.experimental.pallas import tpu as pltpu
from jax.sharding import Mesh
from jax.sharding import PartitionSpec as P

EPSILON = 1e-06
BIG = 8
OUTER = ("big", "zh", "zn")
INNER = ("xt", "xu")
GROUP = (*OUTER, *INNER, "head")
FAR = ("big", "zh")
EIGHT = ("zn", *INNER)


def at(place, sizes):
    index = 0
    for p, s in zip(place, sizes):
        index = index * s + p
    return index


def places(sizes):
    if not sizes:
        yield ()
        return
    for first in range(sizes[0]):
        for rest in places(sizes[1:]):
            yield (first, *rest)


def swapped(value, axes):
    n = lax.axis_size(axes)
    return lax.ppermute(value, axes, [(i, n - 1 - i) for i in range(n)])


def around(value, axes, shift):
    n = lax.axis_size(axes)
    return lax.ppermute(value, axes, [(i, (i + shift) % n) for i in range(n)])


def modulate_body(tok_ref, scale_ref, shift_ref, rider_ref, out_ref):
    values = tok_ref[...].astype(jnp.float32)
    width = values.shape[1]
    center = jnp.mean(values, axis=-1, keepdims=True)
    spread = jnp.mean(jnp.square(values - center), axis=-1, keepdims=True)
    normed = (values - center) / jnp.sqrt(spread + EPSILON)
    out_ref[:, :width] = (normed * (1.0 + scale_ref[...]) + shift_ref[...]).astype(jnp.bfloat16)
    out_ref[:, width:] = rider_ref[...]


def modulate(tokens, scale_mod, shift_mod, rider):
    return pl.pallas_call(
        modulate_body,
        out_shape=jax.ShapeDtypeStruct(
            (tokens.shape[0], tokens.shape[1] + rider.shape[1]), jnp.bfloat16
        ),
        name="modulate",
    )(tokens, scale_mod, shift_mod, rider)


def project_body(order_ref, *refs, parts, pieces, head_dim):
    toks, w_refs = refs[:parts], refs[parts : parts + pieces]
    qg_ref, kg_ref, q_ref, kv_ref = refs[parts + pieces :]
    depth = w_refs[0].shape[-2]

    def norm(shaped, gain):
        mean_square = jnp.mean(jnp.square(shaped), axis=-1, keepdims=True)
        return (shaped / jnp.sqrt(mean_square + EPSILON) * gain).astype(jnp.bfloat16)

    row = 0
    for tok in toks:
        acc, k = None, 0
        for w_ref in w_refs:
            for s in range(w_ref.shape[0]):
                start = pl.multiple_of(order_ref[k] * depth, 128)
                term = jnp.dot(
                    tok[:, pl.ds(start, depth)], w_ref[s], preferred_element_type=jnp.float32
                )
                acc, k = term if acc is None else acc + term, k + 1
        mine = slice(row, row + tok.shape[0])
        q_ref[mine, :] = norm(acc[:, :head_dim], qg_ref[...])
        kv_ref[mine, :head_dim] = norm(acc[:, head_dim : 2 * head_dim], kg_ref[...])
        kv_ref[mine, head_dim:] = acc[:, 2 * head_dim :].astype(jnp.bfloat16)
        row += tok.shape[0]


def project(order, toks, weights, query_gain, key_gain, head_dim):
    rows = sum(t.shape[0] for t in toks)
    vmem = pl.BlockSpec(memory_space=pltpu.VMEM)
    smem = pl.BlockSpec(memory_space=pltpu.SMEM)
    return pl.pallas_call(
        lambda *refs: project_body(
            *refs, parts=len(toks), pieces=len(weights), head_dim=head_dim
        ),
        in_specs=[smem] + [vmem] * (len(toks) + len(weights) + 2),
        out_shape=(
            jax.ShapeDtypeStruct((rows, head_dim), jnp.bfloat16),
            jax.ShapeDtypeStruct((rows, 2 * head_dim), jnp.bfloat16),
        ),
        name="project",
    )(order, *toks, *weights, query_gain[None], key_gain[None])


def attend_body(q_ref, *refs, head_dim, chunk):
    *kv_refs, out_ref, score_ref = refs
    root = math.sqrt(head_dim)
    q = q_ref[...]
    top, at_key, spots = None, 0, []
    for kv in kv_refs:
        step = min(chunk, kv.shape[0])
        for start in range(0, kv.shape[0], step):
            keys = kv[start : start + step, :head_dim]
            s = (
                lax.dot_general(
                    q, keys, (((1,), (1,)), ((), ())), preferred_element_type=jnp.float32
                )
                / root
            )
            score_ref[:, at_key : at_key + step] = s
            m = jnp.max(s, axis=-1, keepdims=True)
            top = m if top is None else jnp.maximum(top, m)
            spots.append((kv, start, at_key, step))
            at_key += step
    total, acc = None, None
    for kv, start, spot, step in spots:
        w = jnp.exp(score_ref[:, spot : spot + step] - top)
        part = jnp.sum(w, axis=-1, keepdims=True)
        term = jnp.dot(
            w.astype(jnp.bfloat16),
            kv[start : start + step, head_dim:],
            preferred_element_type=jnp.float32,
        )
        total = part if total is None else total + part
        acc = term if acc is None else acc + term
    out_ref[...] = (acc / total).astype(jnp.bfloat16)


def attend(query, kvs, head_dim):
    rows = 128
    keys = sum(kv.shape[0] for kv in kvs)
    whole = [pl.BlockSpec(kv.shape, lambda i: (0, 0)) for kv in kvs]
    return pl.pallas_call(
        lambda *refs: attend_body(*refs, head_dim=head_dim, chunk=512),
        grid=(query.shape[0] // rows,),
        in_specs=[pl.BlockSpec((rows, head_dim), lambda i: (i, 0))] + whole,
        out_specs=pl.BlockSpec((rows, head_dim), lambda i: (i, 0)),
        scratch_shapes=[pltpu.VMEM((rows, keys), jnp.float32)],
        out_shape=jax.ShapeDtypeStruct(query.shape, jnp.bfloat16),
        name="attend",
    )(query, *kvs)


def combine_body(order_ref, mixed_ref, *refs):
    *w_refs, gate_ref, out_ref = refs
    summed, k = None, 0
    for w_ref in w_refs:
        depth = w_ref.shape[-1]
        for s in range(w_ref.shape[0]):
            start = pl.multiple_of(order_ref[k] * depth, 128)
            term = lax.dot_general(
                mixed_ref[:, pl.ds(start, depth)],
                w_ref[s],
                (((1,), (1,)), ((), ())),
                preferred_element_type=jnp.float32,
            )
            term = term.astype(jnp.bfloat16).astype(jnp.float32)
            summed, k = term if summed is None else summed + term, k + 1
    out_ref[...] = (summed * gate_ref[...]).astype(jnp.bfloat16)


def combine(order, mixed, weights, gate):
    vmem = pl.BlockSpec(memory_space=pltpu.VMEM)
    smem = pl.BlockSpec(memory_space=pltpu.SMEM)
    return pl.pallas_call(
        combine_body,
        in_specs=[smem] + [vmem] * (len(weights) + 2),
        out_shape=jax.ShapeDtypeStruct((mixed.shape[0], gate.shape[1]), jnp.bfloat16),
        name="combine",
    )(order, mixed, *weights, gate)


def weights_to_tile(packed, sizes):
    turn, move = [], []
    for b, zh, zn, xt, xu, c in places(sizes):
        here = at((b, zh, zn, xt, xu, c), sizes)
        pt, pu = xt ^ (b % 2), xu ^ zn
        there = at((b, zh, zn, pt, pu, c), sizes)
        group = at((xt, xu, c), sizes[3:])
        turn.append((here, there))
        move.append((there, at((group, zh, b // 2 % 2, pt, pu, b // 4), sizes)))
    moved = lax.ppermute(packed, GROUP, turn)
    moved = lax.ppermute(moved, GROUP, move)
    tiles = sizes[1] * sizes[4]
    spare = tiles - moved.shape[0]
    moved = jnp.concatenate([moved, jnp.zeros((spare, *moved.shape[1:]), moved.dtype)], axis=0)
    mine = lax.all_to_all(moved, ("zh", "xu"), 0, 0, tiled=True)
    mine = mine.reshape(sizes[1], sizes[4], *packed.shape[1:])
    odd = lax.axis_index("big") // sizes[5] % 2 == 1
    return jnp.where(odd, mine[:, ::-1], mine).reshape(1, -1, packed.shape[-1])


def per_device(
    tokens,
    shift_mod,
    scale_mod,
    gate_mod,
    query_weight,
    key_weight,
    value_weight,
    out_weight,
    query_gain,
    key_gain,
):
    head_dim = query_gain.shape[0]
    sizes = tuple(lax.axis_size(a) for a in GROUP)
    far, inner, head = lax.axis_size(FAR), lax.axis_size(INNER), sizes[5]
    clips, own, width = tokens.shape
    local_cols = query_weight.shape[1]
    head_count = local_cols // head_dim
    big, zn, xt, xu, zc = (lax.axis_index(a) for a in ("big", "zn", "xt", "xu", "head"))
    zx = lax.axis_index(INNER)

    rider = out_weight.T.reshape(own, -1)
    modulated = modulate(tokens.reshape(own, width), scale_mod, shift_mod, rider)
    gathered = lax.all_gather(modulated, FAR, axis=0, tiled=True)
    mine = gathered[:, :width]
    half = mine.shape[0] // 2
    left = around(mine[:half], INNER, 1)
    right = around(mine[half:], INNER, -1)

    packed = jnp.stack(
        [
            jnp.concatenate(
                [w[:, i * head_dim : (i + 1) * head_dim] for w in (query_weight, key_weight, value_weight)],
                axis=1,
            )
            for i in range(head_count)
        ]
    )
    piece = weights_to_tile(packed, sizes)
    near = [piece, swapped(piece, "zn"), swapped(piece, "xt"), None]
    near[3] = lax.ppermute(piece, ("zn", "xt"), [(i, 3 - i) for i in range(4)])
    stack = jnp.concatenate(near, axis=0)
    weights = [stack, swapped(stack, "head")]
    odd_t = big // (2 * head)
    spot = [(xt ^ t ^ odd_t) + 2 * (zn ^ n) for n, t in ((0, 0), (1, 0), (0, 1), (1, 1))]
    order = jnp.stack([s + 4 * c for c in (zc, 1 - zc) for s in spot]).astype(jnp.int32)

    def exchanged(kv):
        near = [kv, swapped(kv, "zn"), swapped(kv, "xt")]
        near.append(lax.ppermute(kv, ("zn", "xt"), [(i, 3 - i) for i in range(4)]))
        return [*near, swapped(jnp.concatenate(near), "head")]

    query_a, kv_a = project(order, [mine], weights, query_gain, key_gain, head_dim)
    kvs = exchanged(kv_a)
    query_b, kv_b = project(order, [left, right], weights, query_gain, key_gain, head_dim)
    kvs = kvs + exchanged(kv_b)
    heads_out = attend(jnp.concatenate([query_a, query_b]), kvs, head_dim)

    ours, to_left, to_right = heads_out[: 2 * half], heads_out[2 * half : 3 * half], heads_out[3 * half :]
    theirs = jnp.concatenate([around(to_left, INNER, -1), around(to_right, INNER, 1)])
    pair = jnp.where(
        xu == 0, jnp.concatenate([ours, theirs], axis=1), jnp.concatenate([theirs, ours], axis=1)
    )
    back = lax.all_to_all(pair.reshape(far, own, 2 * head_dim), FAR, 0, 0, tiled=True)
    back = back.reshape(sizes[0], sizes[1], own, 2, head_dim)
    back = jnp.transpose(back, (2, 0, 1, 3, 4)).reshape(own, sizes[0], -1)[:, :, :local_cols]
    mixed = lax.all_gather(back.reshape(own, width), EIGHT, axis=0, tiled=True)

    out_far, _ = lax.optimization_barrier((gathered[:, width:], heads_out))
    out_far = out_far.reshape(-1, out_weight.shape[0])
    block = out_far.shape[0] // inner
    got = []
    for s in range(inner):
        send = lax.dynamic_slice_in_dim(out_far, (zx + s) % inner * block, block, axis=0)
        got.append((around(send, INNER, s) if s else send)[None])
    outs = jnp.concatenate(got, axis=0)
    outs = [outs, swapped(outs, "head")]
    source = [(zx - s) % inner * head for s in range(inner)]
    out_order = jnp.stack([s + c for c in (zc, 1 - zc) for s in source]).astype(jnp.int32)
    gate = gate_mod.reshape(inner, far // inner, sizes[2], -1)
    gate = lax.dynamic_index_in_dim(gate, zx, 0, keepdims=False)
    gate = lax.dynamic_index_in_dim(gate, zn, 1, keepdims=False).reshape(1, block)
    done = combine(out_order, mixed, outs, gate)
    done = lax.all_to_all(done.reshape(-1, own, block), EIGHT, 0, 0, tiled=True)
    done = done.reshape(sizes[2], inner, own, far // inner, -1)
    return jnp.transpose(done, (2, 1, 3, 0, 4)).reshape(clips, own, width)


def solution(mesh):
    shape = mesh.shape
    inner = shape["inner"]
    split = (shape["clip"], BIG, 2, shape["outer"] // (2 * BIG), 2, inner // 2, shape["head"])
    fine = Mesh(mesh.devices.reshape(split), ("clip", *GROUP))
    row = (*INNER, "head")
    in_specs = (
        P("clip", GROUP, None),
        P("clip", None),
        P("clip", None),
        P("clip", None),
        P(OUTER, row),
        P(OUTER, row),
        P(OUTER, row),
        P(row, OUTER),
        P(),
        P(),
    )

    return jax.shard_map(
        per_device,
        mesh=fine,
        in_specs=in_specs,
        out_specs=P("clip", GROUP, None),
        check_vma=False,
    )
```

```python
import math

import jax
import jax.numpy as jnp
from jax import lax
from jax.experimental import pallas as pl
from jax.experimental.pallas import tpu as pltpu
from jax.sharding import Mesh
from jax.sharding import PartitionSpec as P

EPSILON = 1e-06
BIG = 8
OUTER = ("big", "zh", "zn")
INNER = ("xt", "xu")
GROUP = (*OUTER, *INNER, "head")
FAR = ("big", "zh")
EIGHT = ("zn", *INNER)


def at(place, sizes):
    index = 0
    for p, s in zip(place, sizes):
        index = index * s + p
    return index


def places(sizes):
    if not sizes:
        yield ()
        return
    for first in range(sizes[0]):
        for rest in places(sizes[1:]):
            yield (first, *rest)


def swapped(value, axes):
    n = lax.axis_size(axes)
    return lax.ppermute(value, axes, [(i, n - 1 - i) for i in range(n)])


def around(value, axes, shift):
    n = lax.axis_size(axes)
    return lax.ppermute(value, axes, [(i, (i + shift) % n) for i in range(n)])


def modulate_body(tok_ref, scale_ref, shift_ref, out_ref):
    values = tok_ref[...].astype(jnp.float32)
    center = jnp.mean(values, axis=-1, keepdims=True)
    spread = jnp.mean(jnp.square(values - center), axis=-1, keepdims=True)
    normed = (values - center) / jnp.sqrt(spread + EPSILON)
    out_ref[...] = (normed * (1.0 + scale_ref[...]) + shift_ref[...]).astype(jnp.bfloat16)


def modulate(tokens, scale_mod, shift_mod):
    return pl.pallas_call(
        modulate_body,
        out_shape=jax.ShapeDtypeStruct(tokens.shape, jnp.bfloat16),
        name="modulate",
    )(tokens, scale_mod, shift_mod)


def project_body(order_ref, *refs, parts, pieces, head_dim):
    toks, w_refs = refs[:parts], refs[parts : parts + pieces]
    qg_ref, kg_ref, q_ref, kv_ref = refs[parts + pieces :]
    depth = w_refs[0].shape[-2]

    def norm(shaped, gain):
        mean_square = jnp.mean(jnp.square(shaped), axis=-1, keepdims=True)
        return (shaped / jnp.sqrt(mean_square + EPSILON) * gain).astype(jnp.bfloat16)

    row = 0
    for tok in toks:
        acc, k = None, 0
        for w_ref in w_refs:
            for s in range(w_ref.shape[0]):
                start = pl.multiple_of(order_ref[k] * depth, 128)
                term = jnp.dot(
                    tok[:, pl.ds(start, depth)], w_ref[s], preferred_element_type=jnp.float32
                )
                acc, k = term if acc is None else acc + term, k + 1
        mine = slice(row, row + tok.shape[0])
        q_ref[mine, :] = norm(acc[:, :head_dim], qg_ref[...])
        kv_ref[mine, :head_dim] = norm(acc[:, head_dim : 2 * head_dim], kg_ref[...])
        kv_ref[mine, head_dim:] = acc[:, 2 * head_dim :].astype(jnp.bfloat16)
        row += tok.shape[0]


def project(order, toks, weights, query_gain, key_gain, head_dim):
    rows = sum(t.shape[0] for t in toks)
    vmem = pl.BlockSpec(memory_space=pltpu.VMEM)
    smem = pl.BlockSpec(memory_space=pltpu.SMEM)
    return pl.pallas_call(
        lambda *refs: project_body(
            *refs, parts=len(toks), pieces=len(weights), head_dim=head_dim
        ),
        in_specs=[smem] + [vmem] * (len(toks) + len(weights) + 2),
        out_shape=(
            jax.ShapeDtypeStruct((rows, head_dim), jnp.bfloat16),
            jax.ShapeDtypeStruct((rows, 2 * head_dim), jnp.bfloat16),
        ),
        name="project",
    )(order, *toks, *weights, query_gain[None], key_gain[None])


def attend_body(q_ref, *refs, head_dim, chunk):
    *kv_refs, out_ref, score_ref = refs
    root = math.sqrt(head_dim)
    q = q_ref[...]
    top, at_key, spots = None, 0, []
    for kv in kv_refs:
        step = min(chunk, kv.shape[0])
        for start in range(0, kv.shape[0], step):
            keys = kv[start : start + step, :head_dim]
            s = (
                lax.dot_general(
                    q, keys, (((1,), (1,)), ((), ())), preferred_element_type=jnp.float32
                )
                / root
            )
            score_ref[:, at_key : at_key + step] = s
            m = jnp.max(s, axis=-1, keepdims=True)
            top = m if top is None else jnp.maximum(top, m)
            spots.append((kv, start, at_key, step))
            at_key += step
    total, acc = None, None
    for kv, start, spot, step in spots:
        w = jnp.exp(score_ref[:, spot : spot + step] - top)
        part = jnp.sum(w, axis=-1, keepdims=True)
        term = jnp.dot(
            w.astype(jnp.bfloat16),
            kv[start : start + step, head_dim:],
            preferred_element_type=jnp.float32,
        )
        total = part if total is None else total + part
        acc = term if acc is None else acc + term
    out_ref[...] = (acc / total).astype(jnp.bfloat16)


def attend(query, kvs, head_dim):
    rows = 128
    keys = sum(kv.shape[0] for kv in kvs)
    whole = [pl.BlockSpec(kv.shape, lambda i: (0, 0)) for kv in kvs]
    return pl.pallas_call(
        lambda *refs: attend_body(*refs, head_dim=head_dim, chunk=512),
        grid=(query.shape[0] // rows,),
        in_specs=[pl.BlockSpec((rows, head_dim), lambda i: (i, 0))] + whole,
        out_specs=pl.BlockSpec((rows, head_dim), lambda i: (i, 0)),
        scratch_shapes=[pltpu.VMEM((rows, keys), jnp.float32)],
        out_shape=jax.ShapeDtypeStruct(query.shape, jnp.bfloat16),
        name="attend",
    )(query, *kvs)


def combine_body(order_ref, mixed_ref, *refs):
    *w_refs, gate_ref, out_ref = refs
    summed, k = None, 0
    for w_ref in w_refs:
        depth = w_ref.shape[-1]
        for s in range(w_ref.shape[0]):
            start = pl.multiple_of(order_ref[k] * depth, 128)
            term = lax.dot_general(
                mixed_ref[:, pl.ds(start, depth)],
                w_ref[s],
                (((1,), (1,)), ((), ())),
                preferred_element_type=jnp.float32,
            )
            term = term.astype(jnp.bfloat16).astype(jnp.float32)
            summed, k = term if summed is None else summed + term, k + 1
    out_ref[...] = (summed * gate_ref[...]).astype(jnp.bfloat16)


def combine(order, mixed, weights, gate):
    vmem = pl.BlockSpec(memory_space=pltpu.VMEM)
    smem = pl.BlockSpec(memory_space=pltpu.SMEM)
    return pl.pallas_call(
        combine_body,
        in_specs=[smem] + [vmem] * (len(weights) + 2),
        out_shape=jax.ShapeDtypeStruct((mixed.shape[0], gate.shape[1]), jnp.bfloat16),
        name="combine",
    )(order, mixed, *weights, gate)


def weights_to_tile(packed, sizes):
    turn, move = [], []
    for b, zh, zn, xt, xu, c in places(sizes):
        here = at((b, zh, zn, xt, xu, c), sizes)
        pt, pu = xt ^ (b % 2), xu ^ zn
        there = at((b, zh, zn, pt, pu, c), sizes)
        group = at((xt, xu, c), sizes[3:])
        turn.append((here, there))
        move.append((there, at((group, zh, b // 2 % 2, pt, pu, b // 4), sizes)))
    moved = lax.ppermute(packed, GROUP, turn)
    moved = lax.ppermute(moved, GROUP, move)
    tiles = sizes[1] * sizes[4]
    spare = tiles - moved.shape[0]
    moved = jnp.concatenate([moved, jnp.zeros((spare, *moved.shape[1:]), moved.dtype)], axis=0)
    mine = lax.all_to_all(moved, ("zh", "xu"), 0, 0, tiled=True)
    mine = mine.reshape(sizes[1], sizes[4], *packed.shape[1:])
    odd = lax.axis_index("big") // sizes[5] % 2 == 1
    return jnp.where(odd, mine[:, ::-1], mine).reshape(1, -1, packed.shape[-1])


def per_device(
    tokens,
    shift_mod,
    scale_mod,
    gate_mod,
    query_weight,
    key_weight,
    value_weight,
    out_weight,
    query_gain,
    key_gain,
):
    head_dim = query_gain.shape[0]
    sizes = tuple(lax.axis_size(a) for a in GROUP)
    far, inner, head = lax.axis_size(FAR), lax.axis_size(INNER), sizes[5]
    clips, own, width = tokens.shape
    local_cols = query_weight.shape[1]
    head_count = local_cols // head_dim
    big, zn, xt, xu, zc = (lax.axis_index(a) for a in ("big", "zn", "xt", "xu", "head"))
    zx = lax.axis_index(INNER)

    modulated = modulate(tokens.reshape(own, width), scale_mod, shift_mod)
    mine = lax.all_gather(modulated, FAR, axis=0, tiled=True)
    half = mine.shape[0] // 2
    left = around(mine[:half], INNER, 1)
    right = around(mine[half:], INNER, -1)

    packed = jnp.stack(
        [
            jnp.concatenate(
                [w[:, i * head_dim : (i + 1) * head_dim] for w in (query_weight, key_weight, value_weight)],
                axis=1,
            )
            for i in range(head_count)
        ]
    )
    piece = weights_to_tile(packed, sizes)
    near = [piece, swapped(piece, "zn"), swapped(piece, "xt"), None]
    near[3] = lax.ppermute(piece, ("zn", "xt"), [(i, 3 - i) for i in range(4)])
    stack = jnp.concatenate(near, axis=0)
    weights = [stack, swapped(stack, "head")]
    odd_t = big // (2 * head)
    spot = [(xt ^ t ^ odd_t) + 2 * (zn ^ n) for n, t in ((0, 0), (1, 0), (0, 1), (1, 1))]
    order = jnp.stack([s + 4 * c for c in (zc, 1 - zc) for s in spot]).astype(jnp.int32)

    query, kv = project(order, [mine, left, right], weights, query_gain, key_gain, head_dim)
    kvs = [kv, swapped(kv, "zn"), swapped(kv, "xt")]
    kvs.append(lax.ppermute(kv, ("zn", "xt"), [(i, 3 - i) for i in range(4)]))
    other = swapped(jnp.concatenate(kvs), "head")
    heads_out = attend(query, [*kvs, other], head_dim)

    ours, to_left, to_right = heads_out[: 2 * half], heads_out[2 * half : 3 * half], heads_out[3 * half :]
    theirs = jnp.concatenate([around(to_left, INNER, -1), around(to_right, INNER, 1)])
    pair = jnp.where(
        xu == 0, jnp.concatenate([ours, theirs], axis=1), jnp.concatenate([theirs, ours], axis=1)
    )
    back = lax.all_to_all(pair.reshape(far, own, 2 * head_dim), FAR, 0, 0, tiled=True)
    back = back.reshape(sizes[0], sizes[1], own, 2, head_dim)
    back = jnp.transpose(back, (2, 0, 1, 3, 4)).reshape(own, sizes[0], -1)[:, :, :local_cols]
    mixed = lax.all_gather(back.reshape(own, width), EIGHT, axis=0, tiled=True)

    out_far = lax.all_gather(out_weight.T, FAR, axis=0, tiled=True)
    out_far, _ = lax.optimization_barrier((out_far, pair))
    block = out_far.shape[0] // inner
    got = []
    for s in range(inner):
        send = lax.dynamic_slice_in_dim(out_far, (zx + s) % inner * block, block, axis=0)
        got.append((around(send, INNER, s) if s else send)[None])
    outs = jnp.concatenate(got, axis=0)
    outs, mixed = lax.optimization_barrier((outs, mixed))
    outs = [outs, swapped(outs, "head")]
    source = [(zx - s) % inner * head for s in range(inner)]
    out_order = jnp.stack([s + c for c in (zc, 1 - zc) for s in source]).astype(jnp.int32)
    gate = gate_mod.reshape(inner, far // inner, sizes[2], -1)
    gate = lax.dynamic_index_in_dim(gate, zx, 0, keepdims=False)
    gate = lax.dynamic_index_in_dim(gate, zn, 1, keepdims=False).reshape(1, block)
    done = combine(out_order, mixed, outs, gate)
    done = lax.all_to_all(done.reshape(-1, own, block), EIGHT, 0, 0, tiled=True)
    done = done.reshape(sizes[2], inner, own, far // inner, -1)
    return jnp.transpose(done, (2, 1, 3, 0, 4)).reshape(clips, own, width)


def solution(mesh):
    shape = mesh.shape
    inner = shape["inner"]
    split = (shape["clip"], BIG, 2, shape["outer"] // (2 * BIG), 2, inner // 2, shape["head"])
    fine = Mesh(mesh.devices.reshape(split), ("clip", *GROUP))
    row = (*INNER, "head")
    in_specs = (
        P("clip", GROUP, None),
        P("clip", None),
        P("clip", None),
        P("clip", None),
        P(OUTER, row),
        P(OUTER, row),
        P(OUTER, row),
        P(row, OUTER),
        P(),
        P(),
    )

    return jax.shard_map(
        per_device,
        mesh=fine,
        in_specs=in_specs,
        out_specs=P("clip", GROUP, None),
        check_vma=False,
    )
```

```python
import math

import jax
import jax.numpy as jnp
from jax import lax
from jax.experimental import pallas as pl
from jax.experimental.pallas import tpu as pltpu
from jax.sharding import Mesh
from jax.sharding import PartitionSpec as P

EPSILON = 1e-06
BIG = 8
OUTER = ("big", "zh", "zn")
INNER = ("xt", "xu")
GROUP = (*OUTER, *INNER, "head")
FAR = ("big", "zh")
EIGHT = ("zn", *INNER)


def at(place, sizes):
    index = 0
    for p, s in zip(place, sizes):
        index = index * s + p
    return index


def places(sizes):
    if not sizes:
        yield ()
        return
    for first in range(sizes[0]):
        for rest in places(sizes[1:]):
            yield (first, *rest)


def swapped(value, axes):
    n = lax.axis_size(axes)
    return lax.ppermute(value, axes, [(i, n - 1 - i) for i in range(n)])


def around(value, axes, shift):
    n = lax.axis_size(axes)
    return lax.ppermute(value, axes, [(i, (i + shift) % n) for i in range(n)])


def modulate_body(tok_ref, scale_ref, shift_ref, out_ref):
    values = tok_ref[...].astype(jnp.float32)
    center = jnp.mean(values, axis=-1, keepdims=True)
    spread = jnp.mean(jnp.square(values - center), axis=-1, keepdims=True)
    normed = (values - center) / jnp.sqrt(spread + EPSILON)
    out_ref[...] = (normed * (1.0 + scale_ref[...]) + shift_ref[...]).astype(jnp.bfloat16)


def modulate(tokens, scale_mod, shift_mod):
    return pl.pallas_call(
        modulate_body,
        out_shape=jax.ShapeDtypeStruct(tokens.shape, jnp.bfloat16),
        name="modulate",
    )(tokens, scale_mod, shift_mod)


def project_body(place_ref, *refs, parts, pieces, head_dim):
    toks, w_refs = refs[:parts], refs[parts : parts + pieces]
    qg_ref, kg_ref, q_ref, kv_ref = refs[parts + pieces :]
    depth = w_refs[0].shape[-2]

    def norm(shaped, gain):
        mean_square = jnp.mean(jnp.square(shaped), axis=-1, keepdims=True)
        return (shaped / jnp.sqrt(mean_square + EPSILON) * gain).astype(jnp.bfloat16)

    row = 0
    for tok in toks:
        acc, k = None, 0
        for w_ref in w_refs:
            for s in range(w_ref.shape[0]):
                start = pl.multiple_of((place_ref[0] ^ k) * depth, 128)
                term = jnp.dot(
                    tok[:, pl.ds(start, depth)], w_ref[s], preferred_element_type=jnp.float32
                )
                acc, k = term if acc is None else acc + term, k + 1
        mine = slice(row, row + tok.shape[0])
        q_ref[mine, :] = norm(acc[:, :head_dim], qg_ref[...])
        kv_ref[mine, :head_dim] = norm(acc[:, head_dim : 2 * head_dim], kg_ref[...])
        kv_ref[mine, head_dim:] = acc[:, 2 * head_dim :].astype(jnp.bfloat16)
        row += tok.shape[0]


def project(place, toks, weights, query_gain, key_gain, head_dim):
    rows = sum(t.shape[0] for t in toks)
    vmem = pl.BlockSpec(memory_space=pltpu.VMEM)
    smem = pl.BlockSpec(memory_space=pltpu.SMEM)
    return pl.pallas_call(
        lambda *refs: project_body(
            *refs, parts=len(toks), pieces=len(weights), head_dim=head_dim
        ),
        in_specs=[smem] + [vmem] * (len(toks) + len(weights) + 2),
        out_shape=(
            jax.ShapeDtypeStruct((rows, head_dim), jnp.bfloat16),
            jax.ShapeDtypeStruct((rows, 2 * head_dim), jnp.bfloat16),
        ),
        name="project",
    )(place, *toks, *weights, query_gain[None], key_gain[None])


def attend_body(q_ref, *refs, head_dim, chunk):
    *kv_refs, out_ref, score_ref = refs
    root = math.sqrt(head_dim)
    q = q_ref[...]
    top, at_key, spots = None, 0, []
    for kv in kv_refs:
        step = min(chunk, kv.shape[0])
        for start in range(0, kv.shape[0], step):
            keys = kv[start : start + step, :head_dim]
            s = (
                lax.dot_general(
                    q, keys, (((1,), (1,)), ((), ())), preferred_element_type=jnp.float32
                )
                / root
            )
            score_ref[:, at_key : at_key + step] = s
            m = jnp.max(s, axis=-1, keepdims=True)
            top = m if top is None else jnp.maximum(top, m)
            spots.append((kv, start, at_key, step))
            at_key += step
    total, acc = None, None
    for kv, start, spot, step in spots:
        w = jnp.exp(score_ref[:, spot : spot + step] - top)
        part = jnp.sum(w, axis=-1, keepdims=True)
        term = jnp.dot(
            w.astype(jnp.bfloat16),
            kv[start : start + step, head_dim:],
            preferred_element_type=jnp.float32,
        )
        total = part if total is None else total + part
        acc = term if acc is None else acc + term
    out_ref[...] = (acc / total).astype(jnp.bfloat16)


def attend(query, kvs, head_dim, first, last):
    rows = 256
    keys = sum(kv.shape[0] for kv in kvs)
    whole = [pl.BlockSpec(kv.shape, lambda i: (0, 0)) for kv in kvs]
    return pl.pallas_call(
        lambda *refs: attend_body(*refs, head_dim=head_dim, chunk=512),
        grid=((last - first) // rows,),
        in_specs=[pl.BlockSpec((rows, head_dim), lambda i: (i + first // rows, 0))] + whole,
        out_specs=pl.BlockSpec((rows, head_dim), lambda i: (i, 0)),
        scratch_shapes=[pltpu.VMEM((rows, keys), jnp.float32)],
        out_shape=jax.ShapeDtypeStruct((last - first, head_dim), jnp.bfloat16),
        name="attend",
    )(query, *kvs)


def combine_body(place_ref, mixed_ref, *refs, head, inner):
    *w_refs, gate_ref, out_ref = refs
    zx, zc, zn = place_ref[0] // (2 * head), place_ref[0] // 2 % head, place_ref[0] % 2
    summed = None
    for side, w_ref in enumerate(w_refs):
        depth = w_ref.shape[-1]
        for s in range(w_ref.shape[0]):
            group = (zx + inner - s) % inner * head + (zc ^ side)
            term = lax.dot_general(
                mixed_ref[:, pl.ds(pl.multiple_of(group * depth, 128), depth)],
                w_ref[s],
                (((1,), (1,)), ((), ())),
                preferred_element_type=jnp.float32,
            )
            term = term.astype(jnp.bfloat16).astype(jnp.float32)
            summed = term if summed is None else summed + term
    step = gate_ref.shape[1]
    parts = out_ref.shape[1] // step
    for f in range(parts):
        gate = gate_ref[pl.ds(2 * (zx * parts + f) + zn, 1), :]
        cols = slice(f * step, (f + 1) * step)
        out_ref[:, cols] = (summed[:, cols] * gate).astype(jnp.bfloat16)


def combine(place, mixed, weights, gate, head, inner):
    vmem = pl.BlockSpec(memory_space=pltpu.VMEM)
    smem = pl.BlockSpec(memory_space=pltpu.SMEM)
    return pl.pallas_call(
        lambda *refs: combine_body(*refs, head=head, inner=inner),
        in_specs=[smem] + [vmem] * (len(weights) + 2),
        out_shape=jax.ShapeDtypeStruct((mixed.shape[0], weights[0].shape[1]), jnp.bfloat16),
        name="combine",
    )(place, mixed, *weights, gate)


def weights_to_tile(packed, sizes):
    turn, move = [], []
    for b, zh, zn, xt, xu, c in places(sizes):
        here = at((b, zh, zn, xt, xu, c), sizes)
        pt, pu = xt ^ (b % 2), xu ^ zn
        there = at((b, zh, zn, pt, pu, c), sizes)
        group = at((xt, xu, c), sizes[3:])
        turn.append((here, there))
        move.append((there, at((group, zh, b // 2 % 2, pt, pu, b // 4), sizes)))
    moved = lax.ppermute(packed, GROUP, turn)
    moved = lax.ppermute(moved, GROUP, move)
    tiles = sizes[1] * sizes[4]
    spare = tiles - moved.shape[0]
    moved = jnp.concatenate([moved, jnp.zeros((spare, *moved.shape[1:]), moved.dtype)], axis=0)
    mine = lax.all_to_all(moved, ("zh", "xu"), 0, 0, tiled=True)
    mine = mine.reshape(sizes[1], sizes[4], *packed.shape[1:])
    odd = lax.axis_index("big") // sizes[5] % 2 == 1
    return jnp.where(odd, mine[:, ::-1], mine).reshape(1, -1, packed.shape[-1])


def per_device(
    tokens,
    shift_mod,
    scale_mod,
    gate_mod,
    query_weight,
    key_weight,
    value_weight,
    out_weight,
    query_gain,
    key_gain,
):
    head_dim = query_gain.shape[0]
    sizes = tuple(lax.axis_size(a) for a in GROUP)
    far, inner, head = lax.axis_size(FAR), lax.axis_size(INNER), sizes[5]
    clips, own, width = tokens.shape
    local_cols = query_weight.shape[1]
    head_count = local_cols // head_dim
    big, zn, xt, xu, zc = (lax.axis_index(a) for a in ("big", "zn", "xt", "xu", "head"))
    zx = lax.axis_index(INNER)

    modulated = modulate(tokens.reshape(own, width), scale_mod, shift_mod)
    mine = lax.all_gather(modulated, FAR, axis=0, tiled=True)
    half = mine.shape[0] // 2
    left = around(mine[:half], INNER, 1)
    right = around(mine[half:], INNER, -1)

    packed = jnp.stack(
        [
            jnp.concatenate(
                [w[:, i * head_dim : (i + 1) * head_dim] for w in (query_weight, key_weight, value_weight)],
                axis=1,
            )
            for i in range(head_count)
        ]
    )
    piece = weights_to_tile(packed, sizes)
    near = [piece, swapped(piece, "xt"), swapped(piece, "zn"), None]
    near[3] = lax.ppermute(piece, ("zn", "xt"), [(i, 3 - i) for i in range(4)])
    stack = jnp.concatenate(near, axis=0)
    weights = [stack, swapped(stack, "head")]
    odd_t = big // (2 * head)
    place = ((xt ^ odd_t) + 2 * zn + 4 * zc).astype(jnp.int32).reshape(1)

    query, kv = project(place, [mine, left, right], weights, query_gain, key_gain, head_dim)
    near = jnp.broadcast_to(kv, (lax.axis_size(("zn", "xt")), *kv.shape))
    near = lax.all_to_all(near, ("zn", "xt"), 0, 0, tiled=True).reshape(-1, kv.shape[1])
    kvs = [near, swapped(near, "head")]
    away = attend(query, kvs, head_dim, 2 * half, 4 * half)
    theirs = [around(away[:half], INNER, -1), around(away[half:], INNER, 1)]
    ours = attend(query, kvs, head_dim, 0, 2 * half)
    theirs = jnp.concatenate(theirs)
    pair = jnp.where(
        xu == 0, jnp.concatenate([ours, theirs], axis=1), jnp.concatenate([theirs, ours], axis=1)
    )
    back = lax.all_to_all(pair.reshape(far, own, 2 * head_dim), FAR, 0, 0, tiled=True)
    back = back.reshape(sizes[0], sizes[1], own, 2, head_dim)
    back = jnp.transpose(back, (2, 0, 1, 3, 4)).reshape(own, sizes[0], -1)[:, :, :local_cols]
    copies = jnp.broadcast_to(back.reshape(own, width), (lax.axis_size(EIGHT), own, width))
    mixed = lax.all_to_all(copies, EIGHT, 0, 0, tiled=True).reshape(-1, width)

    out_far = lax.all_gather(out_weight.T, FAR, axis=0, tiled=True)
    out_far, _ = lax.optimization_barrier((out_far, pair))
    block = out_far.shape[0] // inner
    got = []
    for s in range(inner):
        send = lax.dynamic_slice_in_dim(out_far, (zx + s) % inner * block, block, axis=0)
        got.append((around(send, INNER, s) if s else send)[None])
    outs = jnp.concatenate(got, axis=0)
    outs = [outs, swapped(outs, "head")]
    here = ((zx * head + zc) * 2 + zn).astype(jnp.int32).reshape(1)
    gate = gate_mod.reshape(far * sizes[2], -1)
    done = combine(here, mixed, outs, gate, head, inner)
    done = lax.all_to_all(done.reshape(-1, own, block), EIGHT, 0, 0, tiled=True)
    done = done.reshape(sizes[2], inner, own, far // inner, -1)
    return jnp.transpose(done, (2, 1, 3, 0, 4)).reshape(clips, own, width)


def solution(mesh):
    shape = mesh.shape
    inner = shape["inner"]
    split = (shape["clip"], BIG, 2, shape["outer"] // (2 * BIG), 2, inner // 2, shape["head"])
    fine = Mesh(mesh.devices.reshape(split), ("clip", *GROUP))
    row = (*INNER, "head")
    in_specs = (
        P("clip", GROUP, None),
        P("clip", None),
        P("clip", None),
        P("clip", None),
        P(OUTER, row),
        P(OUTER, row),
        P(OUTER, row),
        P(row, OUTER),
        P(),
        P(),
    )

    return jax.shard_map(
        per_device,
        mesh=fine,
        in_specs=in_specs,
        out_specs=P("clip", GROUP, None),
        check_vma=False,
    )
```

```python
import math

import jax
import jax.numpy as jnp
from jax import lax
from jax.experimental import pallas as pl
from jax.experimental.pallas import tpu as pltpu
from jax.sharding import Mesh
from jax.sharding import PartitionSpec as P

EPSILON = 1e-06
BIG = 8
OUTER = ("big", "zh", "zn")
INNER = ("xt", "xu")
GROUP = (*OUTER, *INNER, "head")
FAR = ("big", "zh")
EIGHT = ("zn", *INNER)


def at(place, sizes):
    index = 0
    for p, s in zip(place, sizes):
        index = index * s + p
    return index


def places(sizes):
    if not sizes:
        yield ()
        return
    for first in range(sizes[0]):
        for rest in places(sizes[1:]):
            yield (first, *rest)


def swapped(value, axes):
    n = lax.axis_size(axes)
    return lax.ppermute(value, axes, [(i, n - 1 - i) for i in range(n)])


def around(value, axes, shift):
    n = lax.axis_size(axes)
    return lax.ppermute(value, axes, [(i, (i + shift) % n) for i in range(n)])


def modulate_body(tok_ref, scale_ref, shift_ref, out_ref):
    values = tok_ref[...].astype(jnp.float32)
    center = jnp.mean(values, axis=-1, keepdims=True)
    spread = jnp.mean(jnp.square(values - center), axis=-1, keepdims=True)
    normed = (values - center) / jnp.sqrt(spread + EPSILON)
    out_ref[...] = (normed * (1.0 + scale_ref[...]) + shift_ref[...]).astype(jnp.bfloat16)


def modulate(tokens, scale_mod, shift_mod):
    return pl.pallas_call(
        modulate_body,
        out_shape=jax.ShapeDtypeStruct(tokens.shape, jnp.bfloat16),
        name="modulate",
    )(tokens, scale_mod, shift_mod)


def project_body(place_ref, *refs, parts, pieces, head_dim):
    toks, w_refs = refs[:parts], refs[parts : parts + pieces]
    qg_ref, kg_ref, q_ref, kv_ref, whole_ref = refs[parts + pieces :]
    depth, k = w_refs[0].shape[-2], 0
    for w_ref in w_refs:
        for s in range(w_ref.shape[0]):
            start = pl.multiple_of((place_ref[0] ^ k) * depth, 128)
            whole_ref[pl.ds(start, depth), :] = w_ref[s]
            k += 1

    def norm(shaped, gain):
        mean_square = jnp.mean(jnp.square(shaped), axis=-1, keepdims=True)
        return (shaped / jnp.sqrt(mean_square + EPSILON) * gain).astype(jnp.bfloat16)

    row = 0
    for tok in toks:
        acc = jnp.dot(tok[...], whole_ref[...], preferred_element_type=jnp.float32)
        mine = slice(row, row + tok.shape[0])
        q_ref[mine, :] = norm(acc[:, :head_dim], qg_ref[...])
        kv_ref[mine, :head_dim] = norm(acc[:, head_dim : 2 * head_dim], kg_ref[...])
        kv_ref[mine, head_dim:] = acc[:, 2 * head_dim :].astype(jnp.bfloat16)
        row += tok.shape[0]


def project(place, toks, weights, query_gain, key_gain, head_dim):
    rows, width = sum(t.shape[0] for t in toks), toks[0].shape[1]
    vmem = pl.BlockSpec(memory_space=pltpu.VMEM)
    smem = pl.BlockSpec(memory_space=pltpu.SMEM)
    return pl.pallas_call(
        lambda *refs: project_body(
            *refs, parts=len(toks), pieces=len(weights), head_dim=head_dim
        ),
        in_specs=[smem] + [vmem] * (len(toks) + len(weights) + 2),
        out_shape=(
            jax.ShapeDtypeStruct((rows, head_dim), jnp.bfloat16),
            jax.ShapeDtypeStruct((rows, 2 * head_dim), jnp.bfloat16),
        ),
        scratch_shapes=[pltpu.VMEM((width, weights[0].shape[-1]), jnp.bfloat16)],
        name="project",
    )(place, *toks, *weights, query_gain[None], key_gain[None])


def attend_body(q_ref, *refs, head_dim, chunk):
    *kv_refs, out_ref, score_ref = refs
    scale = math.log2(math.e) / math.sqrt(head_dim)
    q = q_ref[...]
    top, at_key, spots = None, 0, []
    for kv in kv_refs:
        step = min(chunk, kv.shape[0])
        for start in range(0, kv.shape[0], step):
            keys = kv[start : start + step, :head_dim]
            s = lax.dot_general(
                q, keys, (((1,), (1,)), ((), ())), preferred_element_type=jnp.float32
            )
            score_ref[:, at_key : at_key + step] = s
            m = jnp.max(s, axis=-1, keepdims=True)
            top = m if top is None else jnp.maximum(top, m)
            spots.append((kv, start, at_key, step))
            at_key += step
    total, acc = None, None
    for kv, start, spot, step in spots:
        w = jnp.exp2((score_ref[:, spot : spot + step] - top) * scale)
        part = jnp.sum(w, axis=-1, keepdims=True)
        term = jnp.dot(
            w.astype(jnp.bfloat16),
            kv[start : start + step, head_dim:],
            preferred_element_type=jnp.float32,
        )
        total = part if total is None else total + part
        acc = term if acc is None else acc + term
    out_ref[...] = (acc / total).astype(jnp.bfloat16)


def attend(query, kvs, head_dim, first, last):
    rows = 256
    keys = sum(kv.shape[0] for kv in kvs)
    whole = [pl.BlockSpec(kv.shape, lambda i: (0, 0)) for kv in kvs]
    return pl.pallas_call(
        lambda *refs: attend_body(*refs, head_dim=head_dim, chunk=512),
        grid=((last - first) // rows,),
        in_specs=[pl.BlockSpec((rows, head_dim), lambda i: (i + first // rows, 0))] + whole,
        out_specs=pl.BlockSpec((rows, head_dim), lambda i: (i, 0)),
        scratch_shapes=[pltpu.VMEM((rows, keys), jnp.float32)],
        out_shape=jax.ShapeDtypeStruct((last - first, head_dim), jnp.bfloat16),
        name="attend",
    )(query, *kvs)


def combine_body(place_ref, mixed_ref, *refs, head, inner):
    *w_refs, gate_ref, out_ref = refs
    zx, zc, zn = place_ref[0] // (2 * head), place_ref[0] // 2 % head, place_ref[0] % 2
    summed = None
    for side, w_ref in enumerate(w_refs):
        depth = w_ref.shape[-1]
        for s in range(w_ref.shape[0]):
            group = (zx + inner - s) % inner * head + (zc ^ side)
            term = lax.dot_general(
                mixed_ref[:, pl.ds(pl.multiple_of(group * depth, 128), depth)],
                w_ref[s],
                (((1,), (1,)), ((), ())),
                preferred_element_type=jnp.float32,
            )
            term = term.astype(jnp.bfloat16).astype(jnp.float32)
            summed = term if summed is None else summed + term
    step = gate_ref.shape[1]
    parts = out_ref.shape[1] // step
    for f in range(parts):
        gate = gate_ref[pl.ds(2 * (zx * parts + f) + zn, 1), :]
        cols = slice(f * step, (f + 1) * step)
        out_ref[:, cols] = (summed[:, cols] * gate).astype(jnp.bfloat16)


def combine(place, mixed, weights, gate, head, inner):
    vmem = pl.BlockSpec(memory_space=pltpu.VMEM)
    smem = pl.BlockSpec(memory_space=pltpu.SMEM)
    return pl.pallas_call(
        lambda *refs: combine_body(*refs, head=head, inner=inner),
        in_specs=[smem] + [vmem] * (len(weights) + 2),
        out_shape=jax.ShapeDtypeStruct((mixed.shape[0], weights[0].shape[1]), jnp.bfloat16),
        name="combine",
    )(place, mixed, *weights, gate)


def weights_to_tile(packed, sizes):
    turn, move = [], []
    for b, zh, zn, xt, xu, c in places(sizes):
        here = at((b, zh, zn, xt, xu, c), sizes)
        pt, pu = xt ^ (b % 2), xu ^ zn
        there = at((b, zh, zn, pt, pu, c), sizes)
        group = at((xt, xu, c), sizes[3:])
        turn.append((here, there))
        move.append((there, at((group, zh, b // 2 % 2, pt, pu, b // 4), sizes)))
    moved = lax.ppermute(packed, GROUP, turn)
    moved = lax.ppermute(moved, GROUP, move)
    tiles = sizes[1] * sizes[4]
    spare = tiles - moved.shape[0]
    moved = jnp.concatenate([moved, jnp.zeros((spare, *moved.shape[1:]), moved.dtype)], axis=0)
    mine = lax.all_to_all(moved, ("zh", "xu"), 0, 0, tiled=True)
    mine = mine.reshape(sizes[1], sizes[4], *packed.shape[1:])
    odd = lax.axis_index("big") // sizes[5] % 2 == 1
    return jnp.where(odd, mine[:, ::-1], mine).reshape(1, -1, packed.shape[-1])


def per_device(
    tokens,
    shift_mod,
    scale_mod,
    gate_mod,
    query_weight,
    key_weight,
    value_weight,
    out_weight,
    query_gain,
    key_gain,
):
    head_dim = query_gain.shape[0]
    sizes = tuple(lax.axis_size(a) for a in GROUP)
    far, inner, head = lax.axis_size(FAR), lax.axis_size(INNER), sizes[5]
    clips, own, width = tokens.shape
    local_cols = query_weight.shape[1]
    head_count = local_cols // head_dim
    big, zn, xt, xu, zc = (lax.axis_index(a) for a in ("big", "zn", "xt", "xu", "head"))
    zx = lax.axis_index(INNER)

    modulated = modulate(tokens.reshape(own, width), scale_mod, shift_mod)
    mine = lax.all_gather(modulated, FAR, axis=0, tiled=True)
    half = mine.shape[0] // 2
    left = around(mine[:half], INNER, 1)
    right = around(mine[half:], INNER, -1)

    packed = jnp.stack(
        [
            jnp.concatenate(
                [w[:, i * head_dim : (i + 1) * head_dim] for w in (query_weight, key_weight, value_weight)],
                axis=1,
            )
            for i in range(head_count)
        ]
    )
    piece = weights_to_tile(packed, sizes)
    near = [piece, swapped(piece, "xt"), swapped(piece, "zn"), None]
    near[3] = lax.ppermute(piece, ("zn", "xt"), [(i, 3 - i) for i in range(4)])
    stack = jnp.concatenate(near, axis=0)
    weights = [stack, swapped(stack, "head")]
    odd_t = big // (2 * head)
    place = ((xt ^ odd_t) + 2 * zn + 4 * zc).astype(jnp.int32).reshape(1)

    query, kv = project(place, [mine, left, right], weights, query_gain, key_gain, head_dim)
    near = jnp.broadcast_to(kv, (lax.axis_size(("zn", "xt")), *kv.shape))
    near = lax.all_to_all(near, ("zn", "xt"), 0, 0, tiled=True).reshape(-1, kv.shape[1])
    kvs = [near, swapped(near, "head")]
    away = attend(query, kvs, head_dim, 2 * half, 4 * half)
    theirs = [around(away[:half], INNER, -1), around(away[half:], INNER, 1)]
    ours = attend(query, kvs, head_dim, 0, 2 * half)
    theirs = jnp.concatenate(theirs)
    pair = jnp.where(
        xu == 0, jnp.concatenate([ours, theirs], axis=1), jnp.concatenate([theirs, ours], axis=1)
    )
    back = lax.all_to_all(pair.reshape(far, own, 2 * head_dim), FAR, 0, 0, tiled=True)
    back = back.reshape(sizes[0], sizes[1], own, 2, head_dim)
    back = jnp.transpose(back, (2, 0, 1, 3, 4)).reshape(own, sizes[0], -1)[:, :, :local_cols]
    copies = jnp.broadcast_to(back.reshape(own, width), (lax.axis_size(EIGHT), own, width))
    mixed = lax.all_to_all(copies, EIGHT, 0, 0, tiled=True).reshape(-1, width)

    out_far = lax.all_gather(out_weight.T, FAR, axis=0, tiled=True)
    out_far, _ = lax.optimization_barrier((out_far, pair))
    block = out_far.shape[0] // inner
    got = []
    for s in range(inner):
        send = lax.dynamic_slice_in_dim(out_far, (zx + s) % inner * block, block, axis=0)
        got.append((around(send, INNER, s) if s else send)[None])
    outs = jnp.concatenate(got, axis=0)
    outs = [outs, swapped(outs, "head")]
    here = ((zx * head + zc) * 2 + zn).astype(jnp.int32).reshape(1)
    gate = gate_mod.reshape(far * sizes[2], -1)
    done = combine(here, mixed, outs, gate, head, inner)
    done = lax.all_to_all(done.reshape(-1, own, block), EIGHT, 0, 0, tiled=True)
    done = done.reshape(sizes[2], inner, own, far // inner, -1)
    return jnp.transpose(done, (2, 1, 3, 0, 4)).reshape(clips, own, width)


def solution(mesh):
    shape = mesh.shape
    inner = shape["inner"]
    split = (shape["clip"], BIG, 2, shape["outer"] // (2 * BIG), 2, inner // 2, shape["head"])
    fine = Mesh(mesh.devices.reshape(split), ("clip", *GROUP))
    row = (*INNER, "head")
    in_specs = (
        P("clip", GROUP, None),
        P("clip", None),
        P("clip", None),
        P("clip", None),
        P(OUTER, row),
        P(OUTER, row),
        P(OUTER, row),
        P(row, OUTER),
        P(),
        P(),
    )

    return jax.shard_map(
        per_device,
        mesh=fine,
        in_specs=in_specs,
        out_specs=P("clip", GROUP, None),
        check_vma=False,
    )
```

```python
import math

import jax
import jax.numpy as jnp
from jax import lax
from jax.experimental import pallas as pl
from jax.experimental.pallas import tpu as pltpu
from jax.sharding import Mesh
from jax.sharding import PartitionSpec as P

EPSILON = 1e-06
OUTER = ("big", "zh", "zn")
INNER = ("xt", "xu")
GROUP = (*OUTER, *INNER, "head")
FAR = ("big", "zh")
EIGHT = ("zn", *INNER)


def at(place, sizes):
    index = 0
    for p, s in zip(place, sizes):
        index = index * s + p
    return index


def places(sizes):
    if not sizes:
        yield ()
        return
    for first in range(sizes[0]):
        for rest in places(sizes[1:]):
            yield (first, *rest)


def swapped(value, axes):
    n = lax.axis_size(axes)
    return lax.ppermute(value, axes, [(i, n - 1 - i) for i in range(n)])


def around(value, axes, shift):
    n = lax.axis_size(axes)
    return lax.ppermute(value, axes, [(i, (i + shift) % n) for i in range(n)])


def modulate_body(tok_ref, scale_ref, shift_ref, out_ref):
    values = tok_ref[...].astype(jnp.float32)
    center = jnp.mean(values, axis=-1, keepdims=True)
    spread = jnp.mean(jnp.square(values - center), axis=-1, keepdims=True)
    normed = (values - center) / jnp.sqrt(spread + EPSILON)
    out_ref[...] = (normed * (1.0 + scale_ref[...]) + shift_ref[...]).astype(jnp.bfloat16)


def modulate(tokens, scale_mod, shift_mod):
    return pl.pallas_call(
        modulate_body,
        out_shape=jax.ShapeDtypeStruct(tokens.shape, jnp.bfloat16),
        name="modulate",
    )(tokens, scale_mod, shift_mod)


def project_body(place_ref, *refs, parts, pieces, head_dim):
    toks, w_refs = refs[:parts], refs[parts : parts + pieces]
    qg_ref, kg_ref, q_ref, kv_ref, whole_ref = refs[parts + pieces :]
    depth, k = w_refs[0].shape[-2], 0
    for w_ref in w_refs:
        for s in range(w_ref.shape[0]):
            start = pl.multiple_of((place_ref[0] ^ k) * depth, 128)
            whole_ref[pl.ds(start, depth), :] = w_ref[s]
            k += 1

    def norm(shaped, gain):
        mean_square = jnp.mean(jnp.square(shaped), axis=-1, keepdims=True)
        return (shaped / jnp.sqrt(mean_square + EPSILON) * gain).astype(jnp.bfloat16)

    row = 0
    for tok in toks:
        acc = jnp.dot(tok[...], whole_ref[...], preferred_element_type=jnp.float32)
        mine = slice(row, row + tok.shape[0])
        q_ref[mine, :] = norm(acc[:, :head_dim], qg_ref[...])
        keys = norm(acc[:, head_dim : 2 * head_dim], kg_ref[...])
        values = acc[:, 2 * head_dim :].astype(jnp.bfloat16)
        for copy in range(kv_ref.shape[0]):
            kv_ref[copy, mine, :head_dim] = keys
            kv_ref[copy, mine, head_dim:] = values
        row += tok.shape[0]


def project(place, toks, weights, query_gain, key_gain, head_dim, copies):
    rows, width = sum(t.shape[0] for t in toks), toks[0].shape[1]
    vmem = pl.BlockSpec(memory_space=pltpu.VMEM)
    smem = pl.BlockSpec(memory_space=pltpu.SMEM)
    return pl.pallas_call(
        lambda *refs: project_body(
            *refs, parts=len(toks), pieces=len(weights), head_dim=head_dim
        ),
        in_specs=[smem] + [vmem] * (len(toks) + len(weights) + 2),
        out_shape=(
            jax.ShapeDtypeStruct((rows, head_dim), jnp.bfloat16),
            jax.ShapeDtypeStruct((copies, rows, 2 * head_dim), jnp.bfloat16),
        ),
        scratch_shapes=[pltpu.VMEM((width, weights[0].shape[-1]), jnp.bfloat16)],
        name="project",
    )(place, *toks, *weights, query_gain[None], key_gain[None])


def attend_body(q_ref, *refs, head_dim, chunk):
    *kv_refs, out_ref, score_ref = refs
    scale = math.log2(math.e) / math.sqrt(head_dim)
    q = q_ref[...]
    top, at_key, spots = None, 0, []
    for kv in kv_refs:
        step = min(chunk, kv.shape[0])
        for start in range(0, kv.shape[0], step):
            keys = kv[start : start + step, :head_dim]
            s = lax.dot_general(
                q, keys, (((1,), (1,)), ((), ())), preferred_element_type=jnp.float32
            )
            score_ref[:, at_key : at_key + step] = s
            m = jnp.max(s, axis=-1, keepdims=True)
            top = m if top is None else jnp.maximum(top, m)
            spots.append((kv, start, at_key, step))
            at_key += step
    total, acc = None, None
    for kv, start, spot, step in spots:
        w = jnp.exp2((score_ref[:, spot : spot + step] - top) * scale)
        part = jnp.sum(w, axis=-1, keepdims=True)
        term = jnp.dot(
            w.astype(jnp.bfloat16),
            kv[start : start + step, head_dim:],
            preferred_element_type=jnp.float32,
        )
        total = part if total is None else total + part
        acc = term if acc is None else acc + term
    out_ref[...] = (acc / total).astype(jnp.bfloat16)


def attend(query, kvs, head_dim, first, last):
    rows = 256
    keys = sum(kv.shape[0] for kv in kvs)
    whole = [pl.BlockSpec(memory_space=pltpu.VMEM)] * len(kvs)
    return pl.pallas_call(
        lambda *refs: attend_body(*refs, head_dim=head_dim, chunk=512),
        grid=((last - first) // rows,),
        in_specs=[pl.BlockSpec((rows, head_dim), lambda i: (i + first // rows, 0))] + whole,
        out_specs=pl.BlockSpec((rows, head_dim), lambda i: (i, 0)),
        scratch_shapes=[pltpu.VMEM((rows, keys), jnp.float32)],
        out_shape=jax.ShapeDtypeStruct((last - first, head_dim), jnp.bfloat16),
        name="attend",
    )(query, *kvs)


def combine_body(place_ref, mixed_ref, *refs, head, inner):
    *w_refs, gate_ref, out_ref = refs
    zx, zc, zn = place_ref[0] // (2 * head), place_ref[0] // 2 % head, place_ref[0] % 2
    summed = None
    for side, w_ref in enumerate(w_refs):
        depth = w_ref.shape[-1]
        for s in range(w_ref.shape[0]):
            group = (zx + inner - s) % inner * head + (zc ^ side)
            term = lax.dot_general(
                mixed_ref[:, pl.ds(pl.multiple_of(group * depth, 128), depth)],
                w_ref[s],
                (((1,), (1,)), ((), ())),
                preferred_element_type=jnp.float32,
            )
            term = term.astype(jnp.bfloat16).astype(jnp.float32)
            summed = term if summed is None else summed + term
    step = gate_ref.shape[1]
    parts = out_ref.shape[1] // step
    for f in range(parts):
        gate = gate_ref[pl.ds(2 * (zx * parts + f) + zn, 1), :]
        cols = slice(f * step, (f + 1) * step)
        out_ref[:, cols] = (summed[:, cols] * gate).astype(jnp.bfloat16)


def combine(place, mixed, weights, gate, head, inner):
    vmem = pl.BlockSpec(memory_space=pltpu.VMEM)
    smem = pl.BlockSpec(memory_space=pltpu.SMEM)
    return pl.pallas_call(
        lambda *refs: combine_body(*refs, head=head, inner=inner),
        in_specs=[smem] + [vmem] * (len(weights) + 2),
        out_shape=jax.ShapeDtypeStruct((mixed.shape[0], weights[0].shape[1]), jnp.bfloat16),
        name="combine",
    )(place, mixed, *weights, gate)


def weights_to_tile(packed, sizes):
    turn, move = [], []
    for b, zh, zn, xt, xu, c in places(sizes):
        here = at((b, zh, zn, xt, xu, c), sizes)
        pt, pu = xt ^ (b % 2), xu ^ zn
        there = at((b, zh, zn, pt, pu, c), sizes)
        group = at((xt, xu, c), sizes[3:])
        turn.append((here, there))
        move.append((there, at((group, zh, b // 2 % 2, pt, pu, b // 4), sizes)))
    moved = lax.ppermute(packed, GROUP, turn)
    moved = lax.ppermute(moved, GROUP, move)
    tiles = sizes[1] * sizes[4]
    spare = tiles - moved.shape[0]
    moved = jnp.concatenate([moved, jnp.zeros((spare, *moved.shape[1:]), moved.dtype)], axis=0)
    mine = lax.all_to_all(moved, ("zh", "xu"), 0, 0, tiled=True)
    mine = mine.reshape(sizes[1], sizes[4], *packed.shape[1:])
    odd = lax.axis_index("big") // sizes[5] % 2 == 1
    return jnp.where(odd, mine[:, ::-1], mine).reshape(1, -1, packed.shape[-1])


def per_device(
    tokens,
    shift_mod,
    scale_mod,
    gate_mod,
    query_weight,
    key_weight,
    value_weight,
    out_weight,
    query_gain,
    key_gain,
):
    head_dim = query_gain.shape[0]
    sizes = tuple(lax.axis_size(a) for a in GROUP)
    far, inner, head = lax.axis_size(FAR), lax.axis_size(INNER), sizes[5]
    clips, own, width = tokens.shape
    local_cols = query_weight.shape[1]
    head_count = local_cols // head_dim
    big, zn, xt, xu, zc = (lax.axis_index(a) for a in ("big", "zn", "xt", "xu", "head"))
    zx = lax.axis_index(INNER)

    modulated = modulate(tokens.reshape(own, width), scale_mod, shift_mod)
    mine = lax.all_gather(modulated, FAR, axis=0, tiled=True)
    half = mine.shape[0] // 2
    left = around(mine[:half], INNER, 1)
    right = around(mine[half:], INNER, -1)

    packed = jnp.stack(
        [
            jnp.concatenate(
                [w[:, i * head_dim : (i + 1) * head_dim] for w in (query_weight, key_weight, value_weight)],
                axis=1,
            )
            for i in range(head_count)
        ]
    )
    piece = weights_to_tile(packed, sizes)
    near = [piece, swapped(piece, "xt"), swapped(piece, "zn"), None]
    near[3] = lax.ppermute(piece, ("zn", "xt"), [(i, 3 - i) for i in range(4)])
    stack = jnp.concatenate(near, axis=0)
    weights = [stack, swapped(stack, "head")]
    odd_t = big // (2 * head)
    place = ((xt ^ odd_t) + 2 * zn + 4 * zc).astype(jnp.int32).reshape(1)

    copies = lax.axis_size(("zn", "xt"))
    query, kv = project(
        place, [mine, left, right], weights, query_gain, key_gain, head_dim, copies
    )
    near = lax.all_to_all(kv, ("zn", "xt"), 0, 0, tiled=True).reshape(-1, kv.shape[2])
    kvs = [near, swapped(near, "head")]
    away = attend(query, kvs, head_dim, 2 * half, 4 * half)
    theirs = [around(away[:half], INNER, -1), around(away[half:], INNER, 1)]
    ours = attend(query, kvs, head_dim, 0, 2 * half)
    theirs = jnp.concatenate(theirs)
    pair = jnp.where(
        xu == 0, jnp.concatenate([ours, theirs], axis=1), jnp.concatenate([theirs, ours], axis=1)
    )
    back = lax.all_to_all(pair.reshape(far, own, 2 * head_dim), FAR, 0, 0, tiled=True)
    back = back.reshape(sizes[0], sizes[1], own, 2, head_dim)
    back = jnp.transpose(back, (2, 0, 1, 3, 4)).reshape(own, sizes[0], -1)[:, :, :local_cols]
    copies = jnp.broadcast_to(back.reshape(own, width), (lax.axis_size(EIGHT), own, width))
    mixed = lax.all_to_all(copies, EIGHT, 0, 0, tiled=True).reshape(-1, width)

    out_far = lax.all_gather(out_weight.T, FAR, axis=0, tiled=True)
    out_far, _ = lax.optimization_barrier((out_far, pair))
    block = out_far.shape[0] // inner
    got = []
    for s in range(inner):
        send = lax.dynamic_slice_in_dim(out_far, (zx + s) % inner * block, block, axis=0)
        got.append((around(send, INNER, s) if s else send)[None])
    outs = jnp.concatenate(got, axis=0)
    outs = [outs, swapped(outs, "head")]
    here = ((zx * head + zc) * 2 + zn).astype(jnp.int32).reshape(1)
    gate = gate_mod.reshape(far * sizes[2], -1)
    done = combine(here, mixed, outs, gate, head, inner)
    done = lax.all_to_all(done.reshape(-1, own, block), EIGHT, 0, 0, tiled=True)
    done = done.reshape(sizes[2], inner, own, far // inner, -1)
    return jnp.transpose(done, (2, 1, 3, 0, 4)).reshape(clips, own, width)


def solution(mesh):
    shape = mesh.shape
    inner = shape["inner"]
    big = inner * shape["head"]
    split = (shape["clip"], big, 2, shape["outer"] // (2 * big), 2, inner // 2, shape["head"])
    fine = Mesh(mesh.devices.reshape(split), ("clip", *GROUP))
    row = (*INNER, "head")
    in_specs = (
        P("clip", GROUP, None),
        P("clip", None),
        P("clip", None),
        P("clip", None),
        P(OUTER, row),
        P(OUTER, row),
        P(OUTER, row),
        P(row, OUTER),
        P(),
        P(),
    )

    return jax.shard_map(
        per_device,
        mesh=fine,
        in_specs=in_specs,
        out_specs=P("clip", GROUP, None),
        check_vma=False,
    )
```
